8 devices in a mesh: pod: 1 (over z), data: 2 (over y), tensor: 4 (over x, core).
Axes of the slice: x: 2, y: 2, z: 1, core: 2. Of those that a mesh axis runs over, the one named last changes fastest.
Arguments:
- token_ids: int32 [8192], P(('pod', 'data'))
- embed_table: bfloat16 [49152, 2048], P('tensor')
- norm_gain: bfloat16 [2048], replicated
- w_in: bfloat16 [2048, 8192], P(None, 'tensor')
- w_out: bfloat16 [8192, 2048], P('tensor')
- d_out: bfloat16 [8192, 2048], P(('pod', 'data', 'tensor'))
Outputs:
- output 1: bfloat16 [8192, 2048], P(('pod', 'data', 'tensor'))
- output 2: float32 [49152, 2048], P(('pod', 'tensor'))
- output 3: float32 [2048, 8192], P('pod', 'tensor')
- output 4: float32 [8192, 2048], P(('pod', 'tensor'))
All inputs are finite; a program needn't handle non-finite values.
Results may differ from the reference program's by a relative error of at most 0.00579744.
Values are sent between devices in bfloat16 or wider.
A program may use at most 1 GiB of HBM per device.

```python
import jax
import jax.numpy as jnp
from jax import lax

DATA_WAYS = 2
TENSOR_WAYS = 4
TOK_DEV = 1024
VOCAB_SIZE = 49152
MODEL_DIM = 2048
FFN_DIM = 8192
NORM_EPS = 1e-6
TOKENS_REP = TOK_DEV * TENSOR_WAYS


def gelu_tanh(value):
    return jax.nn.gelu(value, approximate=True)


def draw_ids(id_key):
    k_base, k_shift, k_hot, k_pick, k_use = jax.random.split(id_key, 5)
    total_tok = DATA_WAYS * TOKENS_REP
    base_ids = jax.random.randint(k_base, (total_tok,), 0, VOCAB_SIZE)
    shift_by = jax.random.randint(k_shift, (total_tok,), 0, 3)
    skewed = jnp.right_shift(base_ids, shift_by)
    hot_ids = jax.random.randint(k_hot, (16,), 0, VOCAB_SIZE)
    hot_pick = jax.random.randint(k_pick, (total_tok,), 0, 16)
    use_hot = jax.random.randint(k_use, (total_tok,), 0, 4) == 0
    token_ids = jnp.where(use_hot, hot_ids[hot_pick], skewed)
    token_ids = token_ids.at[0].set(0).at[total_tok - 1].set(VOCAB_SIZE - 1)
    return token_ids.astype(jnp.int32)


def setup_inputs(seed: int = 0, part: int = 0) -> dict:
    root_key = jax.random.key(seed)
    k_table, k_gain, k_in, k_out, k_part = jax.random.split(root_key, 5)
    k_ids, k_grad = jax.random.split(jax.random.fold_in(k_part, part))
    total_tok = DATA_WAYS * TOKENS_REP
    embed_table = jax.random.normal(k_table, (VOCAB_SIZE, MODEL_DIM), jnp.float32).astype(jnp.bfloat16)
    norm_gain = (1.0 + 0.5 * jax.random.uniform(k_gain, (MODEL_DIM,), jnp.float32, -1.0, 1.0)).astype(jnp.bfloat16)
    w_in = (jax.random.normal(k_in, (MODEL_DIM, FFN_DIM), jnp.float32) * MODEL_DIM ** -0.5).astype(jnp.bfloat16)
    w_out = (jax.random.normal(k_out, (FFN_DIM, MODEL_DIM), jnp.float32) * (1.5 * FFN_DIM ** -0.5)).astype(jnp.bfloat16)
    d_out = jax.random.normal(k_grad, (total_tok, MODEL_DIM), jnp.float32).astype(jnp.bfloat16)
    return {"token_ids": draw_ids(k_ids), "embed_table": embed_table, "norm_gain": norm_gain, "w_in": w_in, "w_out": w_out, "d_out": d_out}


def reference(token_ids, embed_table, norm_gain, w_in, w_out, d_out):
    blocks = DATA_WAYS * TENSOR_WAYS
    embedded = jnp.take(embed_table, token_ids, axis=0).reshape(blocks, TOK_DEV, MODEL_DIM)
    grad_blocks = d_out.reshape(blocks, TOK_DEV, MODEL_DIM)
    gain_f32 = norm_gain.astype(jnp.float32)

    def block_step(acc_pair, step_in):
        acc_w_in, acc_w_out = acc_pair
        x_blk, dy_blk = step_in
        x_f32 = x_blk.astype(jnp.float32)
        inv_rms = lax.rsqrt(jnp.mean(x_f32 * x_f32, axis=-1, keepdims=True) + NORM_EPS)
        x_hat = x_f32 * inv_rms
        normed = (x_hat * gain_f32).astype(jnp.bfloat16)
        pre_gelu = jnp.dot(normed, w_in, preferred_element_type=jnp.float32).astype(jnp.bfloat16)
        hidden_f32, gelu_pull = jax.vjp(gelu_tanh, pre_gelu.astype(jnp.float32))
        hidden = hidden_f32.astype(jnp.bfloat16)
        mlp_out = jnp.dot(hidden, w_out, preferred_element_type=jnp.float32)
        out_blk = (x_f32 + mlp_out).astype(jnp.bfloat16)
        grad_hidden = jnp.dot(dy_blk, w_out.T, preferred_element_type=jnp.float32)
        grad_pre = gelu_pull(grad_hidden)[0].astype(jnp.bfloat16)
        acc_w_out = acc_w_out + jnp.dot(hidden.T, dy_blk, preferred_element_type=jnp.float32)
        acc_w_in = acc_w_in + jnp.dot(normed.T, grad_pre, preferred_element_type=jnp.float32)
        d_normed = jnp.dot(grad_pre, w_in.T, preferred_element_type=jnp.float32)
        d_hat = d_normed * gain_f32
        d_norm_in = inv_rms * (d_hat - x_hat * jnp.mean(d_hat * x_hat, axis=-1, keepdims=True))
        dx_blk = (dy_blk.astype(jnp.float32) + d_norm_in).astype(jnp.bfloat16)
        return (acc_w_in, acc_w_out), (out_blk, dx_blk)

    zeros_in = jnp.zeros((MODEL_DIM, FFN_DIM), jnp.float32)
    zeros_out = jnp.zeros((FFN_DIM, MODEL_DIM), jnp.float32)
    (grad_w_in, grad_w_out), (out_blocks, dx_blocks) = lax.scan(block_step, (zeros_in, zeros_out), (embedded, grad_blocks))
    grad_table = jax.ops.segment_sum(dx_blocks.reshape(-1, MODEL_DIM).astype(jnp.float32), token_ids, num_segments=VOCAB_SIZE)
    return out_blocks.reshape(-1, MODEL_DIM), grad_table, grad_w_in, grad_w_out
```

```python
import functools

import jax
import jax.numpy as jnp
from jax import lax
from jax.experimental import pallas as pl
from jax.experimental.pallas import tpu as pltpu
from jax.experimental.layout import Layout, with_layout_constraint
from jax.sharding import PartitionSpec as P


NORM_EPS = 1e-6
LANES = 128
VOCAB_BLOCK = 512
UNROLL = 4
CHUNKS = 2

SWAP_DATA = [(0, 1), (1, 0)]
SWAP_CORE = [(0, 1), (1, 0), (2, 3), (3, 2)]
SWAP_CHIP = [(0, 2), (2, 0), (1, 3), (3, 1)]


def gelu_tanh(value):
    return jax.nn.gelu(value, approximate=True)


def dot_nn(a, b):
    return jnp.dot(a, b, preferred_element_type=jnp.float32)


def dot_nt(a, b):
    return lax.dot_general(a, b, (((1,), (1,)), ((), ())), preferred_element_type=jnp.float32)


def dot_tn(a, b):
    return lax.dot_general(a, b, (((0,), (0,)), ((), ())), preferred_element_type=jnp.float32)


def hidden_and_grad(normed, grad_hidden, w_in):
    pre_gelu = dot_nn(normed, w_in).astype(jnp.bfloat16)
    hidden_f32, gelu_pull = jax.vjp(gelu_tanh, pre_gelu.astype(jnp.float32))
    grad_pre = gelu_pull(grad_hidden)[0].astype(jnp.bfloat16)
    return hidden_f32.astype(jnp.bfloat16), grad_pre


def table_grad_kernel(rows_per_block, token_bits, parts, packed, starts, *refs):
    chunk_refs, (out_ref, rows, acc, sem) = refs[:CHUNKS + 1], refs[CHUNKS + 1:]
    block = pl.program_id(0)

    @pl.when(block == 0)
    def _():
        replica = starts[pl.num_programs(0) + 1]
        copies, at = [], 0
        for k, ref in enumerate(chunk_refs):
            size = ref.shape[0]
            to = pl.multiple_of((replica if k == 0 else 1 - replica) * size, size) if k < 2 else at
            copies.append(pltpu.make_async_copy(ref, rows.at[pl.ds(to, size)], sem.at[k]))
            at += size
        for copy in copies:
            copy.start()
        for copy in copies:
            copy.wait()

    acc[...] = jnp.zeros_like(acc)

    first, last = starts[block], starts[block + 1]
    bulk = (last - first) // UNROLL

    def add_tokens(at, count):
        entries = [packed[at + j] for j in range(count)]
        added = [rows[entry & ((1 << token_bits) - 1)].astype(jnp.float32) for entry in entries]
        for entry, value in zip(entries, added):
            row = (entry >> token_bits) - block * rows_per_block
            to = pl.ds(pl.multiple_of(row * parts, parts), parts)
            acc[to, :] += value

    def add_bulk(i, carry):
        add_tokens(first + i * UNROLL, UNROLL)
        return carry

    def add_rest(i, carry):
        add_tokens(i, 1)
        return carry

    lax.fori_loop(0, bulk, add_bulk, 0)
    lax.fori_loop(first + bulk * UNROLL, last, add_rest, 0)

    def put_rows(group, carry):
        to = pl.ds(pl.multiple_of(group * 8, 8), 8)
        for part in range(parts):
            out_ref[to, part * LANES:(part + 1) * LANES] = acc[pl.ds(group * 8 * parts + part, 8, stride=parts), :]
        return carry

    lax.fori_loop(0, rows_per_block // 8, put_rows, 0)


def table_grad(dx_chunks, packed, starts, shard_rows, token_bits):
    tokens, parts = sum(rows.shape[0] for rows in dx_chunks), dx_chunks[0].shape[1]
    dim = parts * LANES
    return pl.pallas_call(
        functools.partial(table_grad_kernel, VOCAB_BLOCK, token_bits, parts),
        out_shape=jax.ShapeDtypeStruct((shard_rows, dim), jnp.float32),
        grid_spec=pltpu.PrefetchScalarGridSpec(
            num_scalar_prefetch=2,
            grid=(shard_rows // VOCAB_BLOCK,),
            in_specs=[pl.BlockSpec(memory_space=pl.ANY)] * (CHUNKS + 1),
            out_specs=pl.BlockSpec((VOCAB_BLOCK, dim), lambda b, *_: (b, 0)),
            scratch_shapes=[
                pltpu.VMEM((tokens, parts, LANES), jnp.bfloat16),
                pltpu.VMEM((VOCAB_BLOCK * parts, LANES), jnp.float32),
                pltpu.SemaphoreType.DMA((CHUNKS + 1,)),
            ],
        ),
        compiler_params=pltpu.CompilerParams(dimension_semantics=("arbitrary",), vmem_limit_bytes=56 * 1024 * 1024),
        cost_estimate=pl.CostEstimate(flops=100_000_000_000, bytes_accessed=150_000_000, transcendentals=0),
        name="table_grad",
    )(packed, starts, *dx_chunks)


def solution(mesh):
    tok_spec = P(("pod", "data", "tensor"), None)

    def per_device(token_ids, embed_table, norm_gain, w_in, w_out, d_out):
        shard_rows, dim = embed_table.shape
        tok_dev = d_out.shape[0]
        tok_chunk = tok_dev // CHUNKS
        tok_rep = token_ids.shape[0]
        tok_bits = (2 * tok_rep - 1).bit_length()
        half_hid = w_in.shape[1] // 2
        data = lax.axis_index("data")
        rank = lax.axis_index("tensor")
        chip, core = rank // 2, rank % 2
        first_row = rank * shard_rows
        is_first = data == 0

        def pick(to_chip, to_core, k):
            at = (2 * to_chip + to_core) * tok_dev + k * tok_chunk
            ids = lax.dynamic_slice(token_ids, (at,), (tok_chunk,)) - first_row
            owned = (ids >= 0) & (ids < shard_rows)
            rows = jnp.take(embed_table, jnp.where(owned, ids, 0), axis=0, mode="clip")
            return jnp.where(owned[:, None], rows, jnp.zeros_like(rows))

        def gather_group(rows):
            return lax.all_gather(rows, "tensor", axis=0, tiled=True)

        def reduce_group(multiply, rows_all):
            depth = rows_all.shape[1]

            def block(to_chip):
                at = (2 * to_chip + core) * tok_chunk
                return multiply(lax.dynamic_slice(rows_all, (at, 0), (tok_chunk, depth)))

            grid = rows_all.reshape(2, 2, tok_chunk, depth)
            side = multiply(lax.dynamic_slice_in_dim(grid, 1 - core, 1, 1).reshape(2 * tok_chunk, depth))
            side = lax.ppermute(side, "tensor", SWAP_CORE)
            far = block(1 - chip) + lax.dynamic_slice_in_dim(side, (1 - chip) * tok_chunk, tok_chunk, 0)
            far = lax.ppermute(far, "tensor", SWAP_CHIP)
            near = block(chip) + lax.dynamic_slice_in_dim(side, chip * tok_chunk, tok_chunk, 0)
            return near, far

        def far_pair(rows):
            mine = lax.ppermute(rows, "data", SWAP_DATA)
            return mine, lax.ppermute(mine, "tensor", SWAP_CORE)

        def far_block(rows_all):
            rows = lax.dynamic_slice(rows_all, ((2 * (1 - chip) + core) * tok_chunk, 0), (tok_chunk, dim))
            return far_pair(rows)

        grad_dev = [d_out[k * tok_chunk:(k + 1) * tok_chunk] for k in range(CHUNKS)]
        x_dev, rms_dev, normed, grad, normed_near = [], [], [], [], []
        for k in range(CHUNKS):
            grad.append(gather_group(grad_dev[k]))
            far_side = pick(1 - chip, 1 - core, k)
            far_side = lax.ppermute(far_side, "tensor", SWAP_CORE)
            far = pick(1 - chip, core, k) + far_side
            far = lax.ppermute(far, "tensor", SWAP_CHIP)
            near_side = pick(chip, 1 - core, k)
            near_side = lax.ppermute(near_side, "tensor", SWAP_CORE)
            own_rows = pick(chip, core, k)
            gain = norm_gain
            if k:
                far, gain, _ = lax.optimization_barrier((far, norm_gain, rows))
            x_f32 = ((own_rows + near_side) + far).astype(jnp.float32)
            inv_rms = lax.rsqrt(jnp.mean(x_f32 * x_f32, axis=-1, keepdims=True) + NORM_EPS)
            rows = (x_f32 * inv_rms * gain.astype(jnp.float32)).astype(jnp.bfloat16)
            x_dev.append(x_f32)
            rms_dev.append(inv_rms)
            normed.append(gather_group(rows))
            normed_near.append(far_pair(rows))

        grad_far, normed_far = [], []
        for k in range(CHUNKS):
            pieces = list(far_pair(grad_dev[k])) + list(far_block(grad[k]))
            grad_far.append(jnp.concatenate(pieces))
            pieces = list(normed_near[k]) + list(far_block(normed[k]))
            normed_far.append(jnp.concatenate(pieces))

        hidden, grad_pre, d_chunks = [], [], []
        for k in range(CHUNKS):
            if k == 0:
                dh = dot_nt(grad[k], w_out)
                h, du = hidden_and_grad(normed[k], dh, w_in)
            else:
                pre_gelu = dot_nn(normed[k], w_in).astype(jnp.bfloat16)
                h = gelu_tanh(pre_gelu.astype(jnp.float32)).astype(jnp.bfloat16)
                h, pre_gelu, dy = lax.optimization_barrier((h, pre_gelu, grad[k]))
                dh = dot_nt(dy, w_out)
                du = jax.vjp(gelu_tanh, pre_gelu.astype(jnp.float32))[1](dh)[0].astype(jnp.bfloat16)
            hidden.append(h)
            grad_pre.append(du)
            near, far = reduce_group(lambda rows: dot_nt(rows, w_in), du)
            near, far, gain, _ = lax.optimization_barrier((near, far, norm_gain, d_embed if k else near))
            d_normed = near + far
            x_hat = x_dev[k] * rms_dev[k]
            d_hat = d_normed * gain.astype(jnp.float32)
            d_norm_in = rms_dev[k] * (d_hat - x_hat * jnp.mean(d_hat * x_hat, axis=-1, keepdims=True))
            d_embed = (grad_dev[k].astype(jnp.float32) + d_norm_in).astype(jnp.bfloat16)
            d_embed = d_embed.reshape(tok_chunk, dim // LANES, LANES)
            if k == 0:
                d_other = lax.ppermute(d_embed, "data", SWAP_DATA)
                d_chunks.append(gather_group(d_embed))
                d_chunks.append(gather_group(d_other))
            else:
                d_chunks.append(lax.all_gather(d_embed, ("data", "tensor"), axis=0, tiled=True))

        outs = []
        for k in range(CHUNKS):
            near, far = reduce_group(lambda rows: dot_nn(rows, w_out), hidden[k])
            near, far, _ = lax.optimization_barrier((near, far, d_chunks[-1]))
            outs.append((x_dev[k] + (near + far)).astype(jnp.bfloat16))
        block_out = jnp.concatenate(outs)

        other_ids = lax.ppermute(token_ids, "data", SWAP_DATA)
        ids_all = jnp.where(is_first, jnp.concatenate([token_ids, other_ids]), jnp.concatenate([other_ids, token_ids]))
        ids_all = ids_all.reshape(-1, CHUNKS, tok_chunk).transpose(1, 0, 2).reshape(-1)
        local = ids_all - first_row
        key = jnp.where((local >= 0) & (local < shard_rows), local, shard_rows)
        packed = lax.sort((key << tok_bits) | lax.iota(jnp.int32, 2 * tok_rep))
        edges = lax.iota(jnp.int32, shard_rows // VOCAB_BLOCK + 1) * VOCAB_BLOCK
        starts = jnp.sum((key[None, :] < edges[:, None]).astype(jnp.int32), axis=1)
        starts = jnp.concatenate([starts, data.astype(jnp.int32)[None]])
        grad_table = table_grad(d_chunks, packed, starts, shard_rows, tok_bits)

        hid_at = data * half_hid
        w_in_half = lax.dynamic_slice(w_in, (0, hid_at), (dim, half_hid))
        w_out_half = lax.dynamic_slice(w_out, (hid_at, 0), (half_hid, dim))
        g_out = g_in = None
        for k in range(CHUNKS):
            h = lax.dynamic_slice(hidden[k], (0, hid_at), (hidden[k].shape[0], half_hid))
            more = dot_tn(h, grad[k])
            g_out = more if g_out is None else g_out + more
            du = lax.dynamic_slice(grad_pre[k], (0, hid_at), (hidden[k].shape[0], half_hid))
            more = dot_tn(normed[k], du)
            g_in = more if g_in is None else g_in + more
        for k in range(CHUNKS):
            dh = dot_nt(grad_far[k], w_out_half)
            h, du = hidden_and_grad(normed_far[k], dh, w_in_half)
            g_out = g_out + dot_tn(h, grad_far[k])
            g_in = g_in + dot_tn(normed_far[k], du)
        g_in = with_layout_constraint(g_in, Layout(major_to_minor=(0, 1)))
        g_out_other = lax.ppermute(g_out, "data", SWAP_DATA)
        g_in_other = lax.ppermute(g_in, "data", SWAP_DATA)

        def in_order(mine, other, axis):
            both = jnp.concatenate([mine, mine], axis=axis)
            return lax.dynamic_update_slice_in_dim(both, other, (1 - data) * mine.shape[axis], axis)

        grad_w_out = in_order(g_out, g_out_other, 0)
        grad_w_in = in_order(g_in, g_in_other, 1)
        return block_out, grad_table, grad_w_in, grad_w_out

    return jax.shard_map(
        per_device,
        mesh=mesh,
        in_specs=(P(("pod", "data")), P("tensor", None), P(None), P(None, "tensor"), P("tensor", None), tok_spec),
        out_specs=(tok_spec, P(("pod", "tensor"), None), P("pod", "tensor"), P(("pod", "tensor"), None)),
        check_vma=False,
    )
```
